512 devices in a mesh: owner: 64 (over y, x, core), rows: 8 (over z).
Axes of the slice: x: 4, y: 8, z: 8, core: 2. Of those that a mesh axis runs over, the one named last changes fastest.
Arguments:
- train_down: float32 [64, 1024, 2048], P('owner', None, 'rows'), may hold values from -0.1875 to 0.1875
- router_weight: float32 [2048, 64], P('rows', 'owner'), may hold values from -0.125 to 0.125
- router_gain: float32 [2048], P('rows'), may hold values from 0.25 to 1.75
Outputs:
- ready_down: bfloat16 [64, 2048, 1024], P('owner')
- serve_router: bfloat16 [2048, 64], replicated
The draws below stay inside these ranges and needn't reach their ends.
All inputs are finite; a program needn't handle non-finite values.
Results may differ from the reference program's by a relative error of at most 0.001.
Values may be sent and summed in bfloat16 or wider, within the bound.
No kernel may reach another device: no remote copies, remote signals or barrier semaphores. Data moves between devices by JAX's collectives and lax.ppermute only.
A program may use at most 64 MiB of HBM per device.

```python
import jax
import jax.numpy as jnp

EXPERTS = 64
D_MODEL = 2048
D_EXPERT = 1024


def block_levels(key, extent, shards, least, top_value):
    factor_of = 1.0
    for dim, blocks in shards:
        steps = jax.random.uniform(jax.random.fold_in(jax.random.fold_in(key, 6), dim), (blocks,), jnp.float32, least / len(shards), top_value / len(shards))
        factor_of = factor_of * jnp.repeat(jnp.exp(steps), extent[dim] // blocks).reshape((-1,) + (1,) * (len(extent) - 1 - dim))
    return factor_of


def noise(stream_key, shape, spread, most, split=(), dtype=jnp.bfloat16):
    factor_of = block_levels(stream_key, shape, split, -0.22, 0.18) if split else 1.0
    values = jax.random.normal(stream_key, shape, jnp.float32) * spread * factor_of
    return jnp.minimum(jnp.maximum(values, -most), most).astype(dtype)


def setup_inputs(seed: int = 0) -> dict:
    streams_of = jax.random.split(jax.random.key(seed), 4)
    return {
        "train_down": noise(streams_of[0], (EXPERTS, D_EXPERT, D_MODEL), D_EXPERT ** -0.5, 0.1875, ((0, 64), (2, 8)), jnp.float32),
        "router_weight": noise(streams_of[1], (D_MODEL, EXPERTS), D_MODEL ** -0.5, 0.125, ((0, 8), (1, 64)), jnp.float32),
        "router_gain": jnp.clip(1.0 + 0.15 * jax.random.normal(streams_of[2], (D_MODEL,), jnp.float32), 0.25, 1.75),
    }


def reference(train_down, router_weight, router_gain):
    ready_down = train_down.astype(jnp.bfloat16)
    ready_down = jnp.transpose(ready_down, (0, 2, 1))
    serve_router = (router_weight * router_gain[:, None]).astype(jnp.bfloat16)
    return ready_down, serve_router
```

```python
import jax
import jax.numpy as jnp
from jax import lax
from jax.sharding import PartitionSpec as P


def in_order(blocks, dim):
    blocks = jnp.moveaxis(blocks, 0, dim)
    dims = blocks.shape
    return blocks.reshape(*dims[:dim], dims[dim] * dims[dim + 1], *dims[dim + 2 :])


def from_everyone(array, axis):
    copies = jnp.broadcast_to(array, (lax.axis_size(axis), *array.shape))
    return lax.all_to_all(copies, axis, split_axis=0, concat_axis=0, tiled=True)


def gather_directly(array, axis, dim):
    return in_order(from_everyone(array, axis), dim)


def on_device(train_down, router_weight, router_gain):
    n = lax.axis_size("rows")
    z = lax.axis_index("rows")
    right = [(i, (i + 1) % n) for i in range(n)]
    left = [(i, (i - 1) % n) for i in range(n)]
    block = jnp.transpose(train_down[0]).astype(jnp.bfloat16)
    rows, width = block.shape
    half = rows // 2
    out = jnp.zeros((n * rows, width), jnp.bfloat16)
    out = lax.dynamic_update_slice(out, block, (z * rows, 0))
    r = [block[:half], block[half:]]
    l = [block[:half], block[half:]]
    for k in range(1, n // 2 + 1):
        last = k == n // 2
        for c in (0, 1):
            if not (last and c == 1):
                r[c] = lax.ppermute(r[c], "rows", right)
            if not (last and c == 0):
                l[1 - c if False else c] = lax.ppermute(l[c], "rows", left)
        for c in (0, 1):
            if not (last and c == 1):
                out = lax.dynamic_update_slice(out, r[c], (((z - k) % n) * rows + c * half, 0))
            if not (last and c == 0):
                out = lax.dynamic_update_slice(out, l[c], (((z + k) % n) * rows + c * half, 0))
    part_router = (router_weight * router_gain[:, None]).astype(jnp.bfloat16)
    row_router = lax.all_gather(part_router, "rows", axis=0, tiled=True)
    serve_router = gather_directly(row_router, "owner", 1)
    return (out[None], serve_router)


def solution(mesh):
    in_specs = (P("owner", None, "rows"), P("rows", "owner"), P("rows"))
    out_specs = (P("owner", None, None), P())
    return jax.shard_map(
        on_device, mesh=mesh, in_specs=in_specs, out_specs=out_specs, check_vma=False
    )
```

```python
import jax
import jax.numpy as jnp
from jax import lax
from jax.experimental import pallas as pl
from jax.experimental.pallas import tpu as pltpu
from jax.sharding import Mesh
from jax.sharding import PartitionSpec as P


OWNER = ("y", "x", "core")


def a2a(values, axis):
    copies = jnp.broadcast_to(values, (lax.axis_size(axis), *values.shape))
    return lax.all_to_all(copies, axis, split_axis=0, concat_axis=0, tiled=True)


def put(out, arrays, pieces, shape=None):
    count = len(pieces)
    fresh = out is None

    def body(*refs):
        out_ref, sems = refs[-2:]
        n = lax.axis_size("rows")
        rows = out_ref.shape[0] // n
        z, way = lax.axis_index("rows"), 1 - 2 * lax.axis_index("core")
        copies = []
        for i, (which, part, turn) in enumerate(pieces):
            at = pl.multiple_of(((z + turn * way + n) % n) * rows, rows)
            src = refs[which].at[pl.ds(part * rows, rows)]
            copies.append(pltpu.make_async_copy(src, out_ref.at[pl.ds(at, rows)], sems.at[i]))
        for copy in copies:
            copy.start()
        for copy in copies:
            copy.wait()

    arrays = [pltpu.with_memory_space_constraint(a, pltpu.VMEM) for a in arrays]
    whole = pl.BlockSpec(memory_space=pl.ANY)
    return pl.pallas_call(
        body,
        out_shape=jax.ShapeDtypeStruct(shape if fresh else out.shape, jnp.bfloat16),
        in_specs=[pl.BlockSpec(memory_space=pltpu.VMEM)] * len(arrays) + [whole] * (not fresh),
        out_specs=whole,
        scratch_shapes=[pltpu.SemaphoreType.DMA((count,))],
        compiler_params=pltpu.CompilerParams(vmem_limit_bytes=8 << 20),
        input_output_aliases={} if fresh else {len(arrays): 0},
    )(*arrays, *([] if fresh else [out]))


def on_device(train_down, router_weight, router_gain):
    n, g = lax.axis_size("rows"), lax.axis_size(OWNER)
    ax = (*OWNER, "rows")

    def pairs(turn, core):
        out = []
        for a in range(g):
            for i in range(n):
                way = 1 if (a + core) % 2 == 0 else -1
                out.append((a * n + i, (a ^ turn) * n + (i + way) % n))
        return out

    along = pairs(0, 0)
    cross_first = pairs(1, 1)
    cross_last = pairs(1, 0)
    across = [(a * n + i, (a ^ 1) * n + i) for a in range(g) for i in range(n)]

    def send(x, perm):
        return lax.ppermute(x, ax, perm)

    block = jnp.transpose(train_down[0]).astype(jnp.bfloat16)
    rows, width = block.shape

    o1 = send(block, along)
    p1 = send(block, cross_first)
    column = (router_weight[:, 0] * router_gain).astype(jnp.bfloat16).reshape(2, -1)
    column = a2a(column, "rows").reshape(-1, column.shape[1])
    o2 = send(o1, along)
    p2 = send(p1, along)
    table = a2a(column, "y")
    o3 = send(o2, along)
    p3 = send(p2, cross_last)
    table = a2a(table, ("x", "core"))
    table = jnp.swapaxes(table, 0, 1).reshape(g, -1)
    o4 = send(o3, along)
    q1 = send(p1, across)
    q2 = send(p2, across)
    out = put(
        None,
        [block, o1, o2, o3, q1, q2, p3],
        [(0, 0, 0), (1, 0, -1), (2, 0, -2), (3, 0, -3), (4, 0, 1), (5, 0, 2), (6, 0, 3)],
        (n * rows, width),
    )
    out = put(out, [o4], [(0, 0, -4)])
    return (out[None], jnp.transpose(table))


def solution(mesh):
    m = Mesh(mesh.devices.reshape(8, 4, 2, 8), (*OWNER, "rows"))
    in_specs = (P(OWNER, None, "rows"), P("rows", OWNER), P("rows"))
    out_specs = (P(OWNER, None, None), P())
    return jax.shard_map(
        on_device, mesh=m, in_specs=in_specs, out_specs=out_specs, check_vma=False
    )
```

```python
import jax
import jax.numpy as jnp
from jax import lax
from jax.experimental import pallas as pl
from jax.experimental.pallas import tpu as pltpu
from jax.sharding import Mesh
from jax.sharding import PartitionSpec as P


OWNER = ("y", "x", "core")


def a2a(values, axis):
    copies = jnp.broadcast_to(values, (lax.axis_size(axis), *values.shape))
    return lax.all_to_all(copies, axis, split_axis=0, concat_axis=0, tiled=True)


def put(out, arrays, pieces, shape=None):
    count = len(pieces)
    fresh = out is None

    def body(*refs):
        out_ref, sems = refs[-2:]
        n = lax.axis_size("rows")
        rows = out_ref.shape[0] // n
        z, way = lax.axis_index("rows"), 1 - 2 * lax.axis_index("core")
        copies = []
        for i, (which, part, turn) in enumerate(pieces):
            at = pl.multiple_of(((z + turn * way + n) % n) * rows, rows)
            src = refs[which].at[pl.ds(part * rows, rows)]
            copies.append(pltpu.make_async_copy(src, out_ref.at[pl.ds(at, rows)], sems.at[i]))
        for copy in copies:
            copy.start()
        for copy in copies:
            copy.wait()

    arrays = [pltpu.with_memory_space_constraint(a, pltpu.VMEM) for a in arrays]
    whole = pl.BlockSpec(memory_space=pl.ANY)
    return pl.pallas_call(
        body,
        out_shape=jax.ShapeDtypeStruct(shape if fresh else out.shape, jnp.bfloat16),
        in_specs=[pl.BlockSpec(memory_space=pltpu.VMEM)] * len(arrays) + [whole] * (not fresh),
        out_specs=whole,
        scratch_shapes=[pltpu.SemaphoreType.DMA((count,))],
        compiler_params=pltpu.CompilerParams(vmem_limit_bytes=8 << 20),
        input_output_aliases={} if fresh else {len(arrays): 0},
    )(*arrays, *([] if fresh else [out]))


def on_device(train_down, router_weight, router_gain):
    n, g = lax.axis_size("rows"), lax.axis_size(OWNER)
    ax = (*OWNER, "rows")

    def pairs(turn, core):
        out = []
        for a in range(g):
            for i in range(n):
                way = 1 if (a + core) % 2 == 0 else -1
                out.append((a * n + i, (a ^ turn) * n + (i + way) % n))
        return out

    along = pairs(0, 0)
    cross_first = pairs(1, 1)
    cross_last = pairs(1, 0)
    across = [(a * n + i, (a ^ 1) * n + i) for a in range(g) for i in range(n)]

    def send(x, perm):
        return lax.ppermute(x, ax, perm)

    block = jnp.transpose(train_down[0]).astype(jnp.bfloat16)
    rows, width = block.shape

    o1 = send(block, along)
    out = put(None, [block], [(0, 0, 0)], (n * rows, width))
    p1 = send(block, cross_first)
    column = (router_weight[:, 0] * router_gain).astype(jnp.bfloat16).reshape(2, -1)
    table = a2a(column, "y")
    o2 = send(o1, along)
    p2 = send(p1, along)
    table = a2a(table, "rows")
    table = jnp.swapaxes(table, 0, 1).reshape(-1, 2 * n, column.shape[1])
    o3 = send(o2, along)
    p3 = send(p2, cross_last)
    table = a2a(table, ("x", "core"))
    o4 = send(o3, along)
    q1 = send(p1, across)
    q2 = send(p2, across)
    out = put(out, [o1, o2, o3, p3], [(0, 0, -1), (1, 0, -2), (2, 0, -3), (3, 0, 3)])
    table, out = lax.optimization_barrier((table, out))
    out = put(out, [q1, q2], [(0, 0, 1), (1, 0, 2)])
    out = put(out, [o4], [(0, 0, -4)])
    table = jnp.swapaxes(table, 0, 1).reshape(g, -1)
    return (out[None], jnp.transpose(table))


def solution(mesh):
    m = Mesh(mesh.devices.reshape(8, 4, 2, 8), (*OWNER, "rows"))
    in_specs = (P(OWNER, None, "rows"), P("rows", OWNER), P("rows"))
    out_specs = (P(OWNER, None, None), P())
    return jax.shard_map(
        on_device, mesh=m, in_specs=in_specs, out_specs=out_specs, check_vma=False
    )
```

```python
import jax
import jax.numpy as jnp
from jax import lax
from jax.experimental import pallas as pl
from jax.experimental.pallas import tpu as pltpu
from jax.sharding import Mesh
from jax.sharding import PartitionSpec as P


OWNER = ("y", "x", "core")


def a2a(values, axis):
    copies = jnp.broadcast_to(values, (lax.axis_size(axis), *values.shape))
    return lax.all_to_all(copies, axis, split_axis=0, concat_axis=0, tiled=True)


def put(out, arrays, pieces, shape=None):
    count = len(pieces)
    fresh = out is None

    def body(*refs):
        out_ref, sems = refs[-2:]
        n = lax.axis_size("rows")
        rows = out_ref.shape[0] // n
        z, way = lax.axis_index("rows"), 2 * lax.axis_index("core") - 1
        copies = []
        for i, (which, part, turn) in enumerate(pieces):
            at = pl.multiple_of(((z + turn * way + n) % n) * rows, rows)
            src = refs[which].at[pl.ds(part * rows, rows)]
            copies.append(pltpu.make_async_copy(src, out_ref.at[pl.ds(at, rows)], sems.at[i]))
        for copy in copies:
            copy.start()
        for copy in copies:
            copy.wait()

    arrays = [pltpu.with_memory_space_constraint(a, pltpu.VMEM) for a in arrays]
    whole = pl.BlockSpec(memory_space=pl.ANY)
    return pl.pallas_call(
        body,
        out_shape=jax.ShapeDtypeStruct(shape if fresh else out.shape, jnp.bfloat16),
        in_specs=[pl.BlockSpec(memory_space=pltpu.VMEM)] * len(arrays) + [whole] * (not fresh),
        out_specs=whole,
        scratch_shapes=[pltpu.SemaphoreType.DMA((count,))],
        compiler_params=pltpu.CompilerParams(vmem_limit_bytes=8 << 20),
        input_output_aliases={} if fresh else {len(arrays): 0},
    )(*arrays, *([] if fresh else [out]))


def turned(shard, pieces=4):
    inner, rows = shard.shape
    step = inner // pieces

    def body(shard_ref, out_ref, buf, sems):
        copies = [
            pltpu.make_async_copy(shard_ref.at[pl.ds(i * step, step)], buf.at[i], sems.at[i])
            for i in range(pieces)
        ]
        for copy in copies:
            copy.start()
        for i in range(pieces):
            copies[i].wait()
            out_ref[:, i * step : (i + 1) * step] = jnp.transpose(buf[i].astype(jnp.bfloat16))

    return pl.pallas_call(
        body,
        out_shape=jax.ShapeDtypeStruct((rows, inner), jnp.bfloat16),
        in_specs=[pl.BlockSpec(memory_space=pltpu.HBM)],
        out_specs=pl.BlockSpec(memory_space=pltpu.VMEM),
        scratch_shapes=[
            pltpu.VMEM((pieces, step, rows), jnp.float32),
            pltpu.SemaphoreType.DMA((pieces,)),
        ],
        compiler_params=pltpu.CompilerParams(vmem_limit_bytes=8 << 20),
    )(pltpu.with_memory_space_constraint(shard, pltpu.HBM))


def on_device(train_down, router_weight, router_gain):
    n, g = lax.axis_size("rows"), lax.axis_size(OWNER)
    ax = (*OWNER, "rows")

    def pairs(turn, core):
        out = []
        for a in range(g):
            for i in range(n):
                way = -1 if (a + core) % 2 == 0 else 1
                out.append((a * n + i, (a ^ turn) * n + (i + way) % n))
        return out

    along = pairs(0, 0)
    cross_first = pairs(1, 1)
    cross_last = pairs(1, 0)
    across = [(a * n + i, (a ^ 1) * n + i) for a in range(g) for i in range(n)]

    def send(x, perm):
        return lax.ppermute(x, ax, perm)

    block = pltpu.with_memory_space_constraint(turned(train_down[0]), pltpu.VMEM)
    rows, width = block.shape

    o1 = send(block, along)
    out = put(None, [block], [(0, 0, 0)], (n * rows, width))
    p1 = send(block, cross_first)
    column = (router_weight[:, 0] * router_gain).astype(jnp.bfloat16).reshape(2, -1)
    table = a2a(column, "y")
    o2 = send(o1, along)
    p2 = send(p1, along)
    table = a2a(table, "rows")
    table = jnp.swapaxes(table, 0, 1).reshape(-1, 2 * n, column.shape[1])
    o3 = send(o2, along)
    p3 = send(p2, cross_last)
    table = a2a(table, ("x", "core"))
    o4 = send(o3, along)
    q1 = send(p1, across)
    q2 = send(p2, across)
    out = put(out, [o1, o2, o3, p3], [(0, 0, -1), (1, 0, -2), (2, 0, -3), (3, 0, 3)])
    table, out = lax.optimization_barrier((table, out))
    out = put(out, [q1, q2], [(0, 0, 1), (1, 0, 2)])
    out = put(out, [o4], [(0, 0, -4)])
    table = jnp.swapaxes(table, 0, 1).reshape(g, -1)
    return (out[None], jnp.transpose(table))


def solution(mesh):
    m = Mesh(mesh.devices.reshape(8, 4, 2, 8), (*OWNER, "rows"))
    in_specs = (P(OWNER, None, "rows"), P("rows", OWNER), P("rows"))
    out_specs = (P(OWNER, None, None), P())
    return jax.shard_map(
        on_device, mesh=m, in_specs=in_specs, out_specs=out_specs, check_vma=False
    )
```
